128 devices in a mesh: pair: 16 (over x, z_lo, core), ga: 8 (over z_hi, y).
Axes of the slice: x: 4, y: 4, z: 4 (z_hi: 2, z_lo: 2; z = z_hi * 2 + z_lo), core: 2. Of those that a mesh axis runs over, the one named last changes fastest.
Arguments:
- densities: bfloat16 [24576, 4096], P('pair', 'ga'), may hold values from -6 to 6
- val_band: int32 [24576], P('pair'), may hold values from 0 to 127
- cond_band: int32 [24576], P('pair'), may hold values from 0 to 255
- val_energy: float32 [128], replicated, may hold values from -12 to -1
- cond_energy: float32 [256], replicated, may hold values from 1 to 12
Outputs:
- chi: float32 [4096, 4096], P('ga', 'pair')
The draws below stay inside these ranges and needn't reach their ends.
All inputs are finite; a program needn't handle non-finite values.
Results may differ from the reference program's by a relative error of at most 0.0012.
Values may be sent and summed in bfloat16 or wider, within the bound.
A program may use at most 128 MiB of HBM per device.

```python
import math
import jax
import jax.numpy as jnp
from jax import lax

NG = 4096
NV = 128
NC = 256
P_DEV = 1536
PAIRS = 24576
N_PAIR = 16


def place_ends(array, stream_key, least, top_value):
    shape = array.shape
    index_at = [jax.random.randint(jax.random.fold_in(stream_key, axis), (), 0, shape[axis]) for axis in range(len(shape))]
    array = array.at[tuple(index_at)].set(least)
    longest = shape.index(max(shape))
    index_at[longest] = (index_at[longest] + 1) % shape[longest]
    return array.at[tuple(index_at)].set(top_value)


def steps_of(stream_key, shape, cuts, least, high):
    gain, own = 1.0, jax.random.fold_in(stream_key, 6)
    for axis_at, shards_of in cuts:
        heights = jnp.exp(jax.random.uniform(jax.random.fold_in(own, axis_at), (shards_of,), jnp.float32, least / len(cuts), high / len(cuts)))
        gain = gain * jnp.repeat(heights, shape[axis_at] // shards_of).reshape([-1 if axis == axis_at else 1 for axis in range(len(shape))])
    return gain


def gaussian(rng, shape, scale, most, shards=(), held_as=jnp.bfloat16):
    level = steps_of(rng, shape, shards, -0.22, 0.18) if shards else 1.0
    entries = jax.random.normal(rng, shape, jnp.float32) * scale * level
    return jnp.minimum(jnp.maximum(entries, -most), most).astype(held_as)


def setup_inputs(seed: int = 0) -> dict:
    arg_keys = jax.random.split(jax.random.key(seed), 6)
    return {
        "densities": gaussian(arg_keys[0], (PAIRS, NG), 1.0, 6.0, ((0, 16), (1, 8))),
        "val_band": place_ends(jax.random.randint(arg_keys[1], (PAIRS,), 0, NV), jax.random.fold_in(arg_keys[1], 1), 0, NV - 1).astype(jnp.int32),
        "cond_band": place_ends(jax.random.randint(arg_keys[2], (PAIRS,), 0, NC), jax.random.fold_in(arg_keys[2], 1), 0, NC - 1).astype(jnp.int32),
        "val_energy": jnp.clip(jax.random.uniform(arg_keys[3], (NV,), jnp.float32, -12.0, -1.0), -12.0, -1.0),
        "cond_energy": jnp.clip(jax.random.uniform(arg_keys[4], (NC,), jnp.float32, 1.0, 12.0), 1.0, 12.0),
    }


def reference(densities, val_band, cond_band, val_energy, cond_energy):
    gap = val_energy[val_band] - cond_energy[cond_band]
    weight = 4.0 / (gap * math.sqrt(PAIRS))
    scaled = (weight[:, None] * densities.astype(jnp.float32)).astype(jnp.bfloat16)
    left_groups = scaled.reshape(N_PAIR, P_DEV, NG)
    right_groups = densities.reshape(N_PAIR, P_DEV, NG)

    def add_group(total, pieces):
        left, right = pieces
        partial_value = lax.dot_general(left, right, (((0,), (0,)), ((), ())), preferred_element_type=jnp.float32)
        return (total + partial_value, None)
    total, unused = lax.scan(add_group, jnp.zeros((NG, NG), jnp.float32), (left_groups, right_groups))
    return total
```

```python
import math

import jax
import jax.numpy as jnp
from jax import lax
from jax.experimental import pallas as pl
from jax.experimental.pallas import tpu as pltpu
from jax.sharding import PartitionSpec as P

MESH = pl.DeviceIdType.MESH
F32 = jnp.float32
BF16 = jnp.bfloat16
NB = 6


def kernel(
    pairs_total,
    dens, vb, cb, ve, ce,
    out,
    own, y1b, y2b, trb, pb, lo, lp, wt,
    pp, cr, xs0, xr0, xs, xr, xo, tl, lr, fs, fm, db, mb,
    own_sem, y1_s, y1_r, p_s, p_r, tr_s, tr_r, y2_s, y2_r,
    c_s, c_r, x_s, x_r, l_s, l_r, fd_s, fm_s, d_r, m_r,
):
    pair = lax.axis_index("pair")
    g = lax.axis_index("ga")
    x, l, c = pair // 4, (pair // 2) % 2, pair % 2
    h, y = g // 4, g % 4
    kh = y // 2
    y_up, y_dn, y_far = (y + 1) % 4, (y + 3) % 4, (y + 2) % 4

    def remote(src, dst, ss, rs, dev):
        return pltpu.make_async_remote_copy(
            src_ref=src, dst_ref=dst, send_sem=ss, recv_sem=rs, device_id=dev, device_id_type=MESH
        )

    def load_copy(j):
        return pltpu.make_async_copy(
            dens.at[:, :, pl.ds(j * 128, 128)], own.at[j], own_sem.at[j]
        )

    def y1_copy(j):
        return remote(own.at[j], y1b.at[j], y1_s.at[j], y1_r.at[j], (pair, h * 4 + y_dn))

    def p_copy(j):
        return remote(own.at[j], pb.at[j], p_s.at[j], p_r.at[j], (pair, (1 - h) * 4 + y))

    def tr_copy(j):
        return remote(own.at[j, 1 - kh], trb.at[j], tr_s.at[j], tr_r.at[j], (pair, h * 4 + y_up))

    def y2_copy(j):
        return remote(trb.at[j], y2b.at[j], y2_s.at[j], y2_r.at[j], (pair, h * 4 + y_up))

    def core_copy(w, j):
        return remote(
            pp.at[w, j], cr.at[w, j // 2], c_s.at[w, j // 2], c_r.at[w, j // 2],
            (x * 4 + l * 2 + 1 - c, g),
        )

    def x_copy(w, jl, d):
        to = (x + d) % 4
        dev = (to * 4 + l * 2 + c, g)
        if isinstance(w, int) and w == 0:
            return remote(xs0.at[jl, to], xr0.at[jl, d - 1], x_s.at[0, jl, d - 1], x_r.at[0, jl, d - 1], dev)
        return remote(xs.at[w - 1, jl, to], xr.at[w - 1, jl, d - 1], x_s.at[w, jl, d - 1], x_r.at[w, jl, d - 1], dev)

    def l_copy(w):
        return remote(tl.at[w, 1 - l], lr.at[w], l_s.at[w], l_r.at[w], (x * 4 + (1 - l) * 2 + c, g))

    def rows_cols(w):
        p_g = (1 - h) * 4 + y
        row = p_g if w >= 4 else g
        col = {0: g, 1: h * 4 + y_up, 2: h * 4 + y_far, 3: p_g, 4: h * 4 + y_up, 5: h * 4 + y_far}[w]
        return row, col

    def direct_copy(w):
        row, col = rows_cols(w)
        return remote(fs.at[w], db.at[x, c], fd_s.at[w], d_r.at[x, c], (2 * col + l, row))

    def mirror_copy(w):
        row, col = rows_cols(w)
        return remote(fm.at[w], mb.at[2 * l + c, x % 2], fm_s.at[w], m_r.at[2 * l + c, x % 2], (2 * row + x // 2, col))

    for j in range(4):
        load_copy(j).start()
    for j in range(4):
        load_copy(j).wait()
        y1_copy(j).start()
        p_copy(j).start()
        tr_copy(j).start()

    level = lax.broadcasted_iota(jnp.int32, (128, 128), 0)
    tv = jnp.broadcast_to(ve[...], (128, 128)).T
    tc0 = jnp.broadcast_to(ce[0:1, :], (128, 128)).T
    tc1 = jnp.broadcast_to(ce[1:2, :], (128, 128)).T
    for k in range(12):
        v_row = vb[k:k + 1, :]
        c_row = cb[k:k + 1, :]
        val = jnp.sum(jnp.where(level == v_row, tv, 0.0), axis=0, keepdims=True)
        con = jnp.sum(
            jnp.where(level == c_row, tc0, 0.0) + jnp.where(level + 128 == c_row, tc1, 0.0),
            axis=0, keepdims=True,
        )
        wt[k:k + 1, :] = 4.0 / ((val - con) * math.sqrt(pairs_total))

    def scale_into(src, j, dst):
        for k in range(12):
            tile = src[j, k // 6, (k % 6) * 128:(k % 6) * 128 + 128, :].astype(F32).T
            tile = (tile * wt[k:k + 1, :]).astype(BF16)
            dst[k // 6, pl.ds(pl.multiple_of(j * 128, 128), 128), (k % 6) * 128:(k % 6) * 128 + 128] = tile

    def dot(a, b):
        return lax.dot_general(a, b, (((1,), (0,)), ((), ())), preferred_element_type=F32)

    def csend(w, j):
        @pl.when(c != j % 2)
        def _():
            core_copy(w, j).start()

    def consume(w, j):
        jl = j // 2

        @pl.when(c == j % 2)
        def _():
            core_copy(w, j).wait_recv()
            total = pp[w, j] + cr[w, jl]
            for i in range(4):
                if w == 0:
                    xs0[jl, i] = total[i * 128:(i + 1) * 128]
                else:
                    xs[w - 1, jl, i] = total[i * 128:(i + 1) * 128].astype(BF16)
            mine = pl.ds(pl.multiple_of(x * 128, 128), 128)
            xo[w, jl] = pp[w, j, mine, :] + cr[w, jl, mine, :]
            for d in (2, 1, 3):
                x_copy(w, jl, d).start()

    def x_reduce(w):
        for jl in range(2):
            for d in (1, 2, 3):
                x_copy(w, jl, d).wait_recv()
            if w == 0:
                tl[w, jl] = xo[w, jl] + xr0[jl, 0] + xr0[jl, 1] + xr0[jl, 2]
            else:
                tl[w, jl] = (
                    xo[w, jl] + xr[w - 1, jl, 0].astype(F32)
                    + xr[w - 1, jl, 1].astype(F32) + xr[w - 1, jl, 2].astype(F32)
                )
        l_copy(w).start()

    def deliver(w):
        l_copy(w).wait_recv()
        total = tl[w, l] + lr[w]
        fs[w] = total
        if w >= 1:
            fm[w] = total.T
            mirror_copy(w).start()
        if w >= 4:
            direct_copy(w).start()
        else:
            row, col = rows_cols(w)

            @pl.when(2 * col + l == pair)
            def _():
                db[x, c] = fs[w]

            @pl.when(2 * col + l != pair)
            def _():
                direct_copy(w).start()

    @pl.loop(0, 4)
    def _(j):
        scale_into(own, j, lo)

    @pl.loop(0, 4)
    def _(j):
        pp[0, j] = dot(lo[0], own[j, 0]) + dot(lo[1], own[j, 1])
        csend(0, j)

    @pl.loop(0, 4)
    def _(j):
        consume(0, j)

    @pl.loop(0, 4)
    def _(k):
        y1_copy(k).wait_recv()
        pp[1, k] = dot(lo[0], y1b[k, 0]) + dot(lo[1], y1b[k, 1])
        csend(1, k)

        @pl.when(k < 2)
        def _():
            for t in range(2):
                tr_copy(2 * k + t).wait_recv()
                y2_copy(2 * k + t).start()

        p_copy(k).wait_recv()
        pp[3, k] = dot(lo[h], pb[k, h])
        csend(3, k)
        scale_into(pb, k, lp)
        consume(1, k)
        y2_copy(k).wait_recv()
        pp[2, k] = dot(lo[kh], y2b[k])
        csend(2, k)
        consume(3, k)
        consume(2, k)

    x_reduce(0)

    @pl.loop(0, 4)
    def _(j):
        pp[4, j] = dot(lp[0], y1b[j, 0]) + dot(lp[1], y1b[j, 1])
        csend(4, j)
        pp[5, j] = dot(lp[kh], y2b[j])
        csend(5, j)

    deliver(0)
    x_reduce(1)
    x_reduce(3)

    @pl.loop(0, 4)
    def _(j):
        consume(4, j)
        consume(5, j)

    x_reduce(2)
    deliver(1)
    deliver(3)
    deliver(2)
    x_reduce(4)
    x_reduce(5)
    deliver(4)
    deliver(5)

    col = pair // 2
    dy = (col % 4 - y + 4) % 4
    dh = jnp.where(col // 4 != h, 1, 0)
    has_d = dy <= 2
    has_m = (dy >= 2) | ((dy == 0) & (dh == 1))
    here = (c == l) & ((dh == 0) | (dy == 0)) & has_d

    for i in range(4):
        for cc in range(2):
            @pl.when(has_d & jnp.logical_not(here & (x == i) & (c == cc)))
            def _(i=i, cc=cc):
                remote(fs.at[0], db.at[i, cc], fd_s.at[0], d_r.at[i, cc], (pair, (1 - h) * 4 + y)).wait_recv()

            @pl.when(has_m)
            def _(i=i, cc=cc):
                remote(fm.at[1], mb.at[i, cc], fm_s.at[1], m_r.at[i, cc], (pair, (1 - h) * 4 + y)).wait_recv()

    def emit(pick):
        for i in range(4):
            for cc in range(2):
                out[i * 128:(i + 1) * 128, cc * 128:(cc + 1) * 128] = pick(i, cc)

    @pl.when(has_d & has_m)
    def _():
        emit(lambda i, cc: db[i, cc] + mb[i, cc])

    @pl.when(has_d & jnp.logical_not(has_m))
    def _():
        emit(lambda i, cc: db[i, cc])

    @pl.when(jnp.logical_not(has_d))
    def _():
        emit(lambda i, cc: mb[i, cc])

    @pl.loop(0, 4)
    def _(j):
        y1_copy(j).wait_send()
        p_copy(j).wait_send()
        tr_copy(j).wait_send()
        y2_copy(j).wait_send()
        for w in range(NB):
            @pl.when(c != j % 2)
            def _(w=w):
                core_copy(w, j).wait_send()

    for w in range(NB):
        for jl in range(2):
            for d in (1, 2, 3):
                x_copy(w, jl, d).wait_send()
        l_copy(w).wait_send()
        if w >= 1:
            mirror_copy(w).wait_send()
        if w >= 4:
            direct_copy(w).wait_send()
        else:
            row, col_w = rows_cols(w)

            @pl.when(2 * col_w + l != pair)
            def _(w=w):
                direct_copy(w).wait_send()


def per_device(densities, val_band, cond_band, val_energy, cond_energy):
    pairs, cols = densities.shape
    pairs_total = pairs * lax.axis_size("pair")
    vm = pltpu.VMEM
    dma = pltpu.SemaphoreType.DMA
    scratch = [
        vm((4, 2, 768, 128), BF16), vm((4, 2, 768, 128), BF16), vm((4, 768, 128), BF16),
        vm((4, 768, 128), BF16), vm((4, 2, 768, 128), BF16),
        vm((2, 512, 768), BF16), vm((2, 512, 768), BF16), vm((12, 128), F32),
        vm((NB, 4, 512, 128), F32), vm((NB, 2, 512, 128), F32),
        vm((2, 4, 128, 128), F32), vm((2, 3, 128, 128), F32),
        vm((NB - 1, 2, 4, 128, 128), BF16), vm((NB - 1, 2, 3, 128, 128), BF16),
        vm((NB, 2, 128, 128), F32), vm((NB, 2, 128, 128), F32), vm((NB, 128, 128), F32),
        vm((NB, 128, 128), F32), vm((NB, 128, 128), F32),
        vm((4, 2, 128, 128), F32), vm((4, 2, 128, 128), F32),
        dma((4,)), dma((4,)), dma((4,)), dma((4,)), dma((4,)), dma((4,)), dma((4,)), dma((4,)), dma((4,)),
        dma((NB, 2)), dma((NB, 2)), dma((NB, 2, 3)), dma((NB, 2, 3)), dma((NB,)), dma((NB,)),
        dma((NB,)), dma((NB,)), dma((4, 2)), dma((4, 2)),
    ]
    in_vmem = pl.BlockSpec(memory_space=pltpu.VMEM)

    def body(*refs):
        kernel(pairs_total, *refs)

    return pl.pallas_call(
        body,
        name="chi",
        out_shape=jax.ShapeDtypeStruct((512, 256), F32),
        in_specs=[pl.BlockSpec(memory_space=pl.ANY)] + [in_vmem] * 4,
        out_specs=in_vmem,
        scratch_shapes=scratch,
        compiler_params=pltpu.CompilerParams(
            has_side_effects=True, vmem_limit_bytes=40 * 1024 * 1024
        ),
    )(
        densities.reshape(2, pairs // 2, cols),
        val_band.reshape(12, 128),
        cond_band.reshape(12, 128),
        val_energy.reshape(1, 128),
        cond_energy.reshape(2, 128),
    )


def solution(mesh):
    placed = (P("pair", "ga"), P("pair"), P("pair"), P(), P())
    return jax.shard_map(
        per_device, mesh=mesh, in_specs=placed, out_specs=P("ga", "pair"), check_vma=False
    )
```

```python
import math

import jax
import jax.numpy as jnp
from jax import lax
from jax.experimental import pallas as pl
from jax.experimental.pallas import tpu as pltpu
from jax.sharding import PartitionSpec as P

MESH = pl.DeviceIdType.MESH
F32 = jnp.float32
BF16 = jnp.bfloat16
NB = 6


def kernel(
    pairs_total,
    dens, vb_in, cb_in, ve_in, ce_in,
    out,
    own, y1b, y2b, trb, pb, lo, lp, wt, vb, cb, ve, ce,
    pp, cr, xs0, xr0, xs, xr, xo, tl, lr, fs, fm, db, mb,
    in_sem, own_sem, y1_s, y1_r, p_s, p_r, tr_s, tr_r, y2_s, y2_r,
    c_s, c_r, x_s, x_r, l_s, l_r, fd_s, fm_s, d_r, m_r,
):
    pair = lax.axis_index("pair")
    g = lax.axis_index("ga")
    x, l, c = pair // 4, (pair // 2) % 2, pair % 2
    h, y = g // 4, g % 4
    kh = y // 2
    y_up, y_dn, y_far = (y + 1) % 4, (y + 3) % 4, (y + 2) % 4
    other = (1 - h) * 4 + y
    scope = jax.named_scope

    def remote(src, dst, ss, rs, dev):
        return pltpu.make_async_remote_copy(
            src_ref=src, dst_ref=dst, send_sem=ss, recv_sem=rs, device_id=dev, device_id_type=MESH
        )

    def load_copy(j):
        return pltpu.make_async_copy(
            dens.at[:, :, pl.ds(j * 128, 128)], own.at[j], own_sem.at[j]
        )

    def small_copy(i):
        src, dst = ((vb_in, vb), (cb_in, cb), (ve_in, ve), (ce_in, ce))[i]
        return pltpu.make_async_copy(src, dst, in_sem.at[i])

    def y1_copy(j):
        return remote(own.at[j], y1b.at[j], y1_s.at[j], y1_r.at[j], (pair, h * 4 + y_dn))

    def p_copy(j):
        return remote(own.at[j], pb.at[j], p_s.at[j], p_r.at[j], (pair, other))

    def tr_copy(j):
        return remote(own.at[j, 1 - kh], trb.at[j], tr_s.at[j], tr_r.at[j], (pair, h * 4 + y_up))

    def y2_copy(j):
        return remote(trb.at[j], y2b.at[j], y2_s.at[j], y2_r.at[j], (pair, h * 4 + y_up))

    def core_copy(w, j, first, n, part):
        rows = pl.ds(first * 128, n * 128)
        return remote(
            pp.at[w, j, rows], cr.at[w, j // 2, rows], c_s.at[w, j // 2, part], c_r.at[w, j // 2, part],
            (x * 4 + l * 2 + 1 - c, g),
        )

    def x_copy(w, jl, to, slot):
        dev = (to * 4 + l * 2 + c, g)
        if w == 0:
            return remote(xs0.at[jl, to], xr0.at[jl, slot], x_s.at[0, jl, to], x_r.at[0, jl, slot], dev)
        return remote(xs.at[w - 1, jl, to], xr.at[w - 1, jl, slot], x_s.at[w, jl, to], x_r.at[w, jl, slot], dev)

    def l_copy(w):
        return remote(tl.at[w, 1 - l], lr.at[w], l_s.at[w], l_r.at[w], (x * 4 + (1 - l) * 2 + c, g))

    def rows_cols(w):
        row = other if w >= 4 else g
        col = {0: g, 1: h * 4 + y_up, 2: h * 4 + y_far, 3: other, 4: h * 4 + y_up, 5: h * 4 + y_far}[w]
        return row, col

    def stays(w):
        row, col = rows_cols(w)
        return 2 * col + l == pair

    def direct_copy(w):
        row, col = rows_cols(w)
        return remote(fs.at[w], db.at[x, c], fd_s.at[w], d_r.at[x, c], (2 * col + l, row))

    def mirror_copy(w):
        row, col = rows_cols(w)
        return remote(fm.at[w], mb.at[2 * l + c, x % 2], fm_s.at[w], m_r.at[2 * l + c, x % 2], (2 * row + x // 2, col))

    col_own = pair // 2
    dy = (col_own % 4 - y + 4) % 4
    dh = jnp.where(col_own // 4 != h, 1, 0)
    has_d = dy <= 2
    has_m = (dy >= 2) | ((dy == 0) & (dh == 1))
    d_here = (dh == 0) | (dy == 0)
    d_plane = jnp.where(d_here, g, other)
    m_plane = jnp.where(dy == 3, h * 4 + y_dn, jnp.where(dy == 2, h * 4 + y_far, other))
    local = (c == l) & d_here & has_d

    for j in range(4):
        load_copy(j).start()
    for i in range(4):
        small_copy(i).start()

    barrier = pltpu.get_barrier_semaphore()

    def greet(dev):
        pl.semaphore_signal(barrier, inc=1, device_id=dev, device_id_type=MESH)

    greet((pair, h * 4 + y_dn))
    greet((pair, h * 4 + y_up))
    greet((pair, other))
    greet((x * 4 + l * 2 + 1 - c, g))
    greet((x * 4 + (1 - l) * 2 + c, g))
    for d in (1, 2, 3):
        greet((((x + d) % 4) * 4 + l * 2 + c, g))
    for i in range(4):
        for cc in range(2):
            @pl.when(has_d & jnp.logical_not(local & (x == i) & (c == cc)))
            def _(i=i, cc=cc):
                greet((i * 4 + c * 2 + cc, d_plane))

            @pl.when(has_m)
            def _(i=i, cc=cc):
                greet(((2 * c + cc) * 4 + i, m_plane))
    expect = 8 + 11
    for w in range(4):
        expect = expect - jnp.where(stays(w), 1, 0)
    with scope("barrier"):
        pl.semaphore_wait(barrier, expect)

    with scope("first_sends"):
        for j in range(4):
            load_copy(j).wait()
            y1_copy(j).start()
            p_copy(j).start()
            if j < 2:
                tr_copy(j).start()

    with scope("weights"):
        for i in range(4):
            small_copy(i).wait()
        level = lax.broadcasted_iota(jnp.int32, (128, 128), 0)
        tv = jnp.broadcast_to(ve[...], (128, 128)).T
        tc0 = jnp.broadcast_to(ce[0:1, :], (128, 128)).T
        tc1 = jnp.broadcast_to(ce[1:2, :], (128, 128)).T
        for k in range(12):
            v_row = vb[k:k + 1, :]
            c_row = cb[k:k + 1, :]
            val = jnp.sum(jnp.where(level == v_row, tv, 0.0), axis=0, keepdims=True)
            con = jnp.sum(
                jnp.where(level == c_row, tc0, 0.0) + jnp.where(level + 128 == c_row, tc1, 0.0),
                axis=0, keepdims=True,
            )
            wt[k:k + 1, :] = 4.0 / ((val - con) * math.sqrt(pairs_total))

    def scale_into(src, j, dst):
        for k in range(12):
            tile = src[j, k // 6, (k % 6) * 128:(k % 6) * 128 + 128, :].astype(F32).T
            tile = (tile * wt[k:k + 1, :]).astype(BF16)
            rows = pl.ds(j * 128 if isinstance(j, int) else pl.multiple_of(j * 128, 128), 128)
            dst[k // 6, rows, (k % 6) * 128:(k % 6) * 128 + 128] = tile

    def dot(a, b):
        return lax.dot_general(a, b, (((1,), (0,)), ((), ())), preferred_element_type=F32)

    def csend(w, j, first=0, n=4, part=0):
        @pl.when(c != j % 2)
        def _():
            core_copy(w, j, first, n, part).start()

    def consume(w, j, first=0, n=4, part=0):
        jl = j // 2

        @pl.when(c == j % 2)
        def _():
            core_copy(w, j, first, n, part).wait_recv()
            for i in range(first, first + n):
                rows = pl.ds(i * 128, 128)

                @pl.when(x == i)
                def _():
                    xo[w, jl] = pp[w, j, rows, :] + cr[w, jl, rows, :]

                @pl.when(x != i)
                def _():
                    total = pp[w, j, rows, :] + cr[w, jl, rows, :]
                    if w == 0:
                        xs0[jl, i] = total
                    else:
                        xs[w - 1, jl, i] = total.astype(BF16)
                    x_copy(w, jl, i, x).start()

    def x_reduce(w, jl):
        for d in (1, 2, 3):
            x_copy(w, jl, 0, (x + d) % 4).wait_recv()
        total = xo[w, jl]
        for d in (1, 2, 3):
            if w == 0:
                total = total + xr0[jl, (x + d) % 4]
            else:
                total = total + xr[w - 1, jl, (x + d) % 4].astype(F32)
        tl[w, jl] = total

        @pl.when(l != jl)
        def _():
            l_copy(w).start()

    def deliver(w, jl):
        @pl.when(l == jl)
        def _():
            l_copy(w).wait_recv()
            total = tl[w, jl] + lr[w]
            fs[w] = total
            if w >= 1:
                fm[w] = total.T
                mirror_copy(w).start()
            if w >= 4:
                direct_copy(w).start()
            else:
                @pl.when(stays(w))
                def _():
                    db[x, c] = total

                @pl.when(jnp.logical_not(stays(w)))
                def _():
                    direct_copy(w).start()

    def forward(j):
        with scope("wait_tr"):
            tr_copy(j).wait_recv()
        y2_copy(j).start()
        if j < 2:
            tr_copy(j + 2).start()

    with scope("scale_own"):
        @pl.loop(0, 4)
        def _(j):
            scale_into(own, j, lo)

    with scope("mm_w0"):
        @pl.loop(0, 4)
        def _(j):
            pp[0, j] = dot(lo[0], own[j, 0]) + dot(lo[1], own[j, 1])
            csend(0, j)

    with scope("cons_w0"):
        @pl.loop(0, 4)
        def _(j):
            consume(0, j)

    forward(0)
    forward(1)

    def shell(w, k):
        right = (lambda j: dot(lp[kh, rows, :], y2b[j])) if w == 5 else (
            lambda j: dot(lp[0, rows, :], y1b[j, 0]) + dot(lp[1, rows, :], y1b[j, 1])
        )
        rows = pl.ds(0, 128 * (k + 1))
        pp[w, k, rows, :] = right(k)
        csend(w, k, 0, k + 1, 0)
        rows = pl.ds(128 * k, 128)
        for j in range(k):
            pp[w, j, rows, :] = right(j)
            csend(w, j, k, 1, k - j)

    def consume_shell(w, k):
        consume(w, k, 0, k + 1, 0)
        for j in range(k):
            consume(w, j, k, 1, k - j)

    for k in range(4):
        with scope("wait_y1"):
            y1_copy(k).wait_recv()
        with scope("mm_w1"):
            pp[1, k] = dot(lo[0], y1b[k, 0]) + dot(lo[1], y1b[k, 1])
            csend(1, k)
        if k in (1, 2):
            forward(k + 1)
        if k == 2:
            for w in (1, 3, 2):
                with scope("xred_early"):
                    x_reduce(w, 0)
        with scope("wait_p"):
            p_copy(k).wait_recv()
        with scope("mm_w3"):
            pp[3, k] = dot(lo[h], pb[k, h])
            csend(3, k)
        with scope("scale_p"):
            scale_into(pb, k, lp)
        with scope("cons1"):
            consume(1, k)
        with scope("mm_w4"):
            shell(4, k)
        with scope("cons3"):
            consume(3, k)
        with scope("wait_y2"):
            y2_copy(k).wait_recv()
        with scope("mm_w2"):
            pp[2, k] = dot(lo[kh], y2b[k])
            csend(2, k)
        with scope("cons4"):
            consume_shell(4, k)
        with scope("mm_w5"):
            shell(5, k)
        with scope("cons2"):
            consume(2, k)
        if k == 0:
            with scope("xred0"):
                x_reduce(0, 0)
                x_reduce(0, 1)
        if k == 1:
            with scope("deliver0"):
                deliver(0, 0)
                deliver(0, 1)
        if k == 2:
            with scope("del_early"):
                for w in (1, 3, 2):
                    deliver(w, 0)
        with scope("cons5"):
            consume_shell(5, k)

    for w in (1, 3, 4, 2, 5):
        for jl in range(2):
            if w >= 4 or jl == 1:
                with scope(f"xred_w{w}"):
                    x_reduce(w, jl)
    for w in (1, 3, 4, 2, 5):
        for jl in range(2):
            if w >= 4 or jl == 1:
                with scope(f"deliver_w{w}"):
                    deliver(w, jl)

    with scope("wait_final"):
        for i in range(4):
            for cc in range(2):
                @pl.when(has_d & jnp.logical_not(local & (x == i) & (c == cc)))
                def _(i=i, cc=cc):
                    remote(fs.at[0], db.at[i, cc], fd_s.at[0], d_r.at[i, cc], (pair, other)).wait_recv()

                @pl.when(has_m)
                def _(i=i, cc=cc):
                    remote(fm.at[1], mb.at[i, cc], fm_s.at[1], m_r.at[i, cc], (pair, other)).wait_recv()

    def emit(pick):
        for i in range(4):
            for cc in range(2):
                out[i * 128:(i + 1) * 128, cc * 128:(cc + 1) * 128] = pick(i, cc)

    with scope("emit"):
        @pl.when(has_d & has_m)
        def _():
            emit(lambda i, cc: db[i, cc] + mb[i, cc])

        @pl.when(has_d & jnp.logical_not(has_m))
        def _():
            emit(lambda i, cc: db[i, cc])

        @pl.when(jnp.logical_not(has_d))
        def _():
            emit(lambda i, cc: mb[i, cc])

    with scope("wait_sends"):
        for j in range(4):
            y1_copy(j).wait_send()
            p_copy(j).wait_send()
            tr_copy(j).wait_send()
            y2_copy(j).wait_send()

            @pl.when(c != j % 2)
            def _(j=j):
                for w in range(4):
                    core_copy(w, j, 0, 4, 0).wait_send()
                for w in (4, 5):
                    core_copy(w, j, 0, j + 1, 0).wait_send()
                    for k in range(j + 1, 4):
                        core_copy(w, j, k, 1, k - j).wait_send()

        for w in range(NB):
            for jl in range(2):
                for d in (1, 2, 3):
                    x_copy(w, jl, (x + d) % 4, x).wait_send()
            l_copy(w).wait_send()
            if w >= 1:
                mirror_copy(w).wait_send()
            if w >= 4:
                direct_copy(w).wait_send()
            else:
                @pl.when(jnp.logical_not(stays(w)))
                def _(w=w):
                    direct_copy(w).wait_send()


def per_device(densities, val_band, cond_band, val_energy, cond_energy):
    pairs, cols = densities.shape
    pairs_total = pairs * lax.axis_size("pair")
    vm = pltpu.VMEM
    dma = pltpu.SemaphoreType.DMA
    scratch = [
        vm((4, 2, 768, 128), BF16), vm((4, 2, 768, 128), BF16), vm((4, 768, 128), BF16),
        vm((4, 768, 128), BF16), vm((4, 2, 768, 128), BF16),
        vm((2, 512, 768), BF16), vm((2, 512, 768), BF16), vm((12, 128), F32),
        vm((12, 128), jnp.int32), vm((12, 128), jnp.int32), vm((1, 128), F32), vm((2, 128), F32),
        vm((NB, 4, 512, 128), F32), vm((NB, 2, 512, 128), F32),
        vm((2, 4, 128, 128), F32), vm((2, 4, 128, 128), F32),
        vm((NB - 1, 2, 4, 128, 128), BF16), vm((NB - 1, 2, 4, 128, 128), BF16),
        vm((NB, 2, 128, 128), F32), vm((NB, 2, 128, 128), F32), vm((NB, 128, 128), F32),
        vm((NB, 128, 128), F32), vm((NB, 128, 128), F32),
        vm((4, 2, 128, 128), F32), vm((4, 2, 128, 128), F32),
        dma((4,)), dma((4,)), dma((4,)), dma((4,)), dma((4,)), dma((4,)), dma((4,)), dma((4,)), dma((4,)), dma((4,)),
        dma((NB, 2, 4)), dma((NB, 2, 4)), dma((NB, 2, 4)), dma((NB, 2, 4)), dma((NB,)), dma((NB,)),
        dma((NB,)), dma((NB,)), dma((4, 2)), dma((4, 2)),
    ]
    in_vmem = pl.BlockSpec(memory_space=pltpu.VMEM)

    def body(*refs):
        kernel(pairs_total, *refs)

    return pl.pallas_call(
        body,
        name="chi",
        out_shape=jax.ShapeDtypeStruct((512, 256), F32),
        in_specs=[pl.BlockSpec(memory_space=pl.ANY)] * 5,
        out_specs=in_vmem,
        scratch_shapes=scratch,
        compiler_params=pltpu.CompilerParams(
            collective_id=0, has_side_effects=True, vmem_limit_bytes=62 * 1024 * 1024
        ),
    )(
        densities.reshape(2, pairs // 2, cols),
        val_band.reshape(12, 128),
        cond_band.reshape(12, 128),
        val_energy.reshape(1, 128),
        cond_energy.reshape(2, 128),
    )


def solution(mesh):
    placed = (P("pair", "ga"), P("pair"), P("pair"), P(), P())
    return jax.shard_map(
        per_device, mesh=mesh, in_specs=placed, out_specs=P("ga", "pair"), check_vma=False
    )
```
